32 devices in a mesh: grp: 8 (over y, x, core), wrk: 4 (over z).
Axes of the slice: x: 2, y: 2, z: 4, core: 2. Of those that a mesh axis runs over, the one named last changes fastest.
Arguments:
- mono_ham: bfloat16 [32, 256, 256], P(('grp', 'wrk')), as said below
- polymer_members: int32 [32, 3], P(('grp', 'wrk')), may hold values from -1 to 31, as said below
- polymer_coupling: bfloat16 [32, 3, 256, 256], P(('grp', 'wrk')), may hold values from -0.29882812 to 0.29882812
Outputs:
- density: float32 [32, 256, 256], P(('grp', 'wrk'))
The draws below stay inside these ranges and needn't reach their ends.
Inputs may be any that keep to these rules, and one draw needn't show every extreme that they name: `mono_ham`: each block is symmetric. `polymer_members`: row p lists distinct members: the first is monomer p itself; the second is another monomer of p's group (p // 4) or a monomer of the next group ((p // 4 + 1) mod 8); the third is -1 for a dimer, else a monomer of the next group.
All inputs are finite; a program needn't handle non-finite values.
Results may differ from the reference program's by a relative error of at most 0.012.
Values may be sent and summed in bfloat16 or wider, within the bound.
No kernel may reach another device: no remote copies, remote signals or barrier semaphores. Data moves between devices by JAX's collectives and lax.ppermute only.
A program may use at most 64 MiB of HBM per device.

```python
import jax
import jax.numpy as jnp
from jax import lax

ORB = 256
ITERS = 2
MONOMERS = 32
POLYMERS = 32
N_GRP = 8
N_WRK = 4


def draw_mono_ham(key, part):
    first, second = jax.random.split(jax.random.fold_in(key, 11))
    noise = jax.random.normal(first, (MONOMERS, ORB, ORB), jnp.float32)
    levels = jax.random.uniform(second, (MONOMERS, ORB), jnp.float32, -0.2, 0.2)
    symmetric = (noise + jnp.swapaxes(noise, 1, 2)) * (0.008 / 1.4142136)
    hamiltonian = symmetric + levels[:, :, None] * jnp.eye(ORB, dtype=jnp.float32)[None, :, :]
    return hamiltonian.astype(jnp.bfloat16)


def draw_polymer_members(key, part):
    keys = jax.random.split(jax.random.fold_in(key, 23), 5)
    total = N_GRP * N_WRK
    device = jnp.arange(total, dtype=jnp.int32)
    own_group = device // N_WRK
    position = device % N_WRK
    next_group = (own_group + 1) % N_GRP
    outward = jax.random.randint(keys[0], (total,), 0, 2)
    step_near = jax.random.randint(keys[1], (total,), 1, N_WRK)
    far_place = jax.random.randint(keys[2], (total,), 0, N_WRK)
    second = jnp.where(outward == 0, own_group * N_WRK + (position + step_near) % N_WRK, next_group * N_WRK + far_place)
    step_far = jax.random.randint(keys[3], (total,), 1, N_WRK)
    third_place = jnp.where(outward == 1, (far_place + step_far) % N_WRK, far_place)
    kinds = jax.random.randint(keys[4], (total,), 0, 4)
    third = jnp.where(kinds == 0, next_group * N_WRK + third_place, -1)
    return jnp.stack([device, second, third], 1).astype(jnp.int32)


def block_scale(own_key, shape, cuts, low, largest):
    def one(axis_at, shards_of):
        steps = jax.random.uniform(jax.random.fold_in(jax.random.fold_in(own_key, 6), axis_at), (shards_of,), jnp.float32, low / len(cuts), largest / len(cuts))
        return jnp.repeat(jnp.exp(steps), shape[axis_at] // shards_of).reshape((-1,) + (1,) * (len(shape) - axis_at - 1))

    level = one(*cuts[0])
    for cut in cuts[1:]:
        level = level * one(*cut)
    return level


def centred(own_key, shape, deviation, reach, shards=(), kind=jnp.bfloat16):
    array = jax.random.normal(own_key, shape, jnp.float32) * deviation
    if len(shards) > 0:
        array = block_scale(own_key, shape, shards, -0.22, 0.18) * array
    return jnp.clip(array, min=-reach, max=reach).astype(kind)


def setup_inputs(seed: int = 0) -> dict:
    key_of = jax.random.split(jax.random.key(seed), 4)
    mono_ham = draw_mono_ham(jax.random.fold_in(key_of[3], 71), 0)
    polymer_members = draw_polymer_members(jax.random.fold_in(key_of[3], 71), 0)
    polymer_coupling = centred(key_of[2], (POLYMERS, 3, ORB, ORB), 0.05, 0.29882812, ((0, 32),))
    return dict(mono_ham=mono_ham, polymer_members=polymer_members, polymer_coupling=polymer_coupling)


def purify_full(density):
    for _ in range(ITERS):
        rounded = density.astype(jnp.bfloat16)
        square = jnp.dot(rounded, rounded, preferred_element_type=jnp.float32)
        product = jnp.dot(square.astype(jnp.bfloat16), rounded, preferred_element_type=jnp.float32)
        density = 3.0 * square - 2.0 * product
    return density


def purify_diagonal(density):
    for _ in range(ITERS - 1):
        rounded = density.astype(jnp.bfloat16)
        square = jnp.dot(rounded, rounded, preferred_element_type=jnp.float32)
        product = jnp.dot(square.astype(jnp.bfloat16), rounded, preferred_element_type=jnp.float32)
        density = 3.0 * square - 2.0 * product
    rounded = density.astype(jnp.bfloat16)
    square = jnp.dot(rounded, rounded, preferred_element_type=jnp.float32)
    square_low = square.astype(jnp.bfloat16)
    diagonal = []
    for position in range(3):
        lower_edge = position * ORB
        upper_edge = lower_edge + ORB
        product = jnp.dot(square_low[lower_edge:upper_edge], rounded[:, lower_edge:upper_edge], preferred_element_type=jnp.float32)
        diagonal.append(3.0 * square[lower_edge:upper_edge, lower_edge:upper_edge] - 2.0 * product)
    return jnp.stack(diagonal)


def polymer_frame(hamiltonians, couplings, third_flag):
    upper_rows = jnp.concatenate([hamiltonians[0], couplings[0], couplings[1]], 1)
    middle_rows = jnp.concatenate([couplings[0].T, hamiltonians[1], couplings[2]], 1)
    lower_rows = jnp.concatenate([couplings[1].T, couplings[2].T, hamiltonians[2]], 1)
    whole_frame = jnp.concatenate([upper_rows, middle_rows, lower_rows], 0)
    identity = jnp.eye(3 * ORB, dtype=jnp.float32)
    keep_mask = jnp.concatenate([jnp.ones((2 * ORB,), jnp.float32), jnp.ones((ORB,), jnp.float32) * third_flag])
    return (0.5 * identity - 0.35 * whole_frame) * keep_mask[:, None] * keep_mask[None, :]


def reference(mono_ham, polymer_members, polymer_coupling):
    identity = jnp.eye(ORB, dtype=jnp.float32)

    def monomer(block):
        return purify_full(0.5 * identity - 0.35 * block.astype(jnp.float32))

    mono_density = lax.map(monomer, mono_ham)

    def polymer(operands):
        members, coupling = operands
        present = members >= 0
        safe_index = jnp.where(present, members, 0).astype(jnp.int32)
        hamiltonians = mono_ham[safe_index].astype(jnp.float32)
        initial = polymer_frame(hamiltonians, coupling.astype(jnp.float32), present[2].astype(jnp.float32))
        diagonal = purify_diagonal(initial)
        lower_order = mono_density[safe_index]
        return ((diagonal - lower_order) * present[:, None, None].astype(jnp.float32)).astype(jnp.bfloat16)

    corrections = lax.map(polymer, (polymer_members, polymer_coupling))

    def collect(running, device):
        own_group = device // N_WRK
        behind = (device - N_WRK) % POLYMERS
        members = jnp.concatenate([polymer_members[device], polymer_members[behind]])
        pieces = jnp.concatenate([corrections[device], corrections[behind]], 0).astype(jnp.float32)
        valid = (members >= 0) & (jnp.floor_divide(members, N_WRK) == own_group)
        targets = jnp.where(members >= 0, members % N_WRK, 0)
        onehot = ((targets[:, None] == jnp.arange(N_WRK, dtype=jnp.int32)[None, :]) & valid[:, None]).astype(jnp.float32)
        partial_value = jnp.einsum("sw,sx->wx", onehot, pieces.reshape(6, ORB * ORB), precision=lax.Precision.HIGHEST)
        rounded = lax.optimization_barrier(partial_value.astype(jnp.bfloat16))
        first_row = (own_group * N_WRK).astype(jnp.int32)
        current = lax.dynamic_slice_in_dim(running, first_row, N_WRK, 0)
        updated = current + rounded.astype(jnp.float32).reshape(N_WRK, ORB, ORB)
        return lax.dynamic_update_slice_in_dim(running, updated, first_row, 0), None

    running = jnp.zeros((MONOMERS, ORB, ORB), jnp.float32)
    running, _ = lax.scan(collect, running, jnp.arange(POLYMERS, dtype=jnp.int32))
    return mono_density + running
```

```python
import jax
import jax.numpy as jnp
from jax import lax
from jax.experimental import pallas as pl
from jax.experimental.pallas import tpu as pltpu
from jax.sharding import PartitionSpec as P


F32 = jnp.float32
BF16 = jnp.bfloat16
PAD = 8


def from_behind(block, axis, distance):
    devices = range(lax.axis_size(axis))
    route = [((i - distance) % len(devices), i) for i in devices]
    return lax.ppermute(block, axis, route)


def dot(a, b):
    return jnp.dot(a, b, preferred_element_type=F32)


def grid_masks(half):
    row = lax.broadcasted_iota(jnp.int32, (half, half), 0)
    col = lax.broadcasted_iota(jnp.int32, (half, half), 1)
    return row, col


def eye(n):
    row, col = grid_masks(n)
    return jnp.where(row == col, 1.0, 0.0)


def pack_into(ref, index, block, code=None):
    n = block.shape[-1]
    half = n // 2
    row, col = grid_masks(half)
    low = block[half:, half:]
    folded = jnp.where(row >= col, block[:half, :half], low)
    diagonal = jnp.sum(jnp.where(row == col, low, 0.0), axis=0, keepdims=True)
    ref[index, :half, :half] = folded.astype(BF16)
    ref[index, :half, half:] = block[:half, half:].astype(BF16)
    tail = jnp.broadcast_to(jnp.concatenate([diagonal, diagonal], 1), (PAD, n))
    if code is not None:
        line = lax.broadcasted_iota(jnp.int32, (PAD, n), 0)
        tail = jnp.where(line == 0, tail, code)
    ref[index, half:, :] = tail.astype(BF16)


def unpack(folded, corner, diagonal):
    half = folded.shape[0]
    row, col = grid_masks(half)
    turned = folded.T
    first = jnp.where(row >= col, folded, turned)
    last = jnp.where(row < col, folded, jnp.where(row > col, turned, diagonal))
    return first, corner, corner.T, last


def purified(low):
    square = dot(low, low)
    density = 3.0 * square - 2.0 * dot(square.astype(BF16), low)
    low = density.astype(BF16)
    square = dot(low, low)
    return 3.0 * square - 2.0 * dot(square.astype(BF16), low)


def pack_kernel(ham, out):
    block = ham[0].astype(F32)
    n = block.shape[-1]
    pack_into(out, 0, 0.5 * eye(n) - 0.35 * block)


def early_kernel(scalars, ham, coupling, frame, known, mono, rows, *, workers):
    n = ham.shape[-1]
    own = (0.5 * eye(n) - 0.35 * ham[0].astype(F32)).astype(BF16)
    third = jnp.where(scalars[2] >= 0, 1.0, 0.0)
    c01 = -0.35 * coupling[0, 0].astype(F32)
    c02 = -0.35 * coupling[0, 1].astype(F32) * third
    c12 = -0.35 * coupling[0, 2].astype(F32) * third
    frame[:n, :n] = own
    frame[:n, n : 2 * n] = c01.astype(BF16)
    frame[:n, 2 * n :] = c02.astype(BF16)
    frame[n : 2 * n, :n] = c01.T.astype(BF16)
    frame[n : 2 * n, n : 2 * n] = jnp.zeros((n, n), BF16)
    frame[n : 2 * n, 2 * n :] = c12.astype(BF16)
    frame[2 * n :, :n] = c02.T.astype(BF16)
    frame[2 * n :, n : 2 * n] = c12.T.astype(BF16)
    frame[2 * n :, 2 * n :] = jnp.zeros((n, n), BF16)
    whole = frame[...]
    for i in range(3):
        known[i * n : (i + 1) * n, :] = dot(whole[i * n : (i + 1) * n, :], whole)
    mono[...] = purified(own)
    group = scalars[3]
    slot = scalars[4]
    groups = scalars[5]
    following = lax.rem(group + 1, groups)
    second, last = scalars[1], scalars[2]
    line = 0

    def put(value):
        nonlocal line
        rows[line, :] = jnp.full((n,), value, F32)
        line += 1

    for k in range(1, workers):
        mate = group * workers + lax.rem(slot + k, workers)
        put(jnp.where(second == mate, 1.0, 0.0))
    for member in (second, last):
        for k in range(workers):
            mate = following * workers + lax.rem(slot + k, workers)
            put(jnp.where(member == mate, 1.0, 0.0))
    inside = (second >= group * workers) & (second < (group + 1) * workers)
    second_slot = lax.rem(second, workers).astype(F32)
    last_slot = jnp.where(last >= 0, lax.rem(last, workers), -1).astype(F32)
    put(jnp.where(inside, second_slot, -1.0))
    put(jnp.where(inside, -1.0, second_slot))
    put(last_slot)
    for k in range(workers):
        put(lax.rem(slot + workers - k, workers).astype(F32))


def main_kernel(*refs, workers):
    own = refs[: workers - 1]
    following = refs[workers - 1 : 2 * workers - 1]
    known_frame, known, mono, rows, going, staying, mine, frame, square_low = refs[2 * workers - 1 :]
    n = mono.shape[-1]
    half = n // 2
    base = 3 * workers - 1

    def chosen(candidates, first_row):
        total = jnp.zeros((half + PAD, n), F32)
        for c, ref in enumerate(candidates):
            total = jnp.where(rows[first_row + c : first_row + c + 1, :] > 0.5, ref[0].astype(F32), total)
        return total

    second = chosen(own + following, 0)
    last = chosen(following, 2 * workers - 1)
    frame[...] = known_frame[...]
    for at, packed in ((1, second), (2, last)):
        parts = unpack(packed[:half, :half], packed[:half, half:], packed[half : half + 1, :half])
        upper_left, upper_right, lower_left, lower_right = parts
        top = at * n
        frame[top : top + half, top : top + half] = upper_left.astype(BF16)
        frame[top : top + half, top + half : top + n] = upper_right.astype(BF16)
        frame[top + half : top + n, top : top + half] = lower_left.astype(BF16)
        frame[top + half : top + n, top + half : top + n] = lower_right.astype(BF16)
    second = frame[n : 2 * n, n : 2 * n]
    last = frame[2 * n :, 2 * n :]
    squares = []
    for i in range(3):
        band = known_frame[i * n : (i + 1) * n, :]
        middle = dot(band[:, n : 2 * n], second)
        right = dot(band[:, 2 * n :], last)
        row = known[i * n : (i + 1) * n, :]
        if i == 0:
            left, middle_extra, right_extra = None, None, None
        else:
            block = second if i == 1 else last
            left = dot(block, known_frame[i * n : (i + 1) * n, :n])
            middle_extra = dot(block, frame[i * n : (i + 1) * n, n : 2 * n])
            right_extra = dot(block, frame[i * n : (i + 1) * n, 2 * n :])
        parts = [row[:, :n], row[:, n : 2 * n] + middle, row[:, 2 * n :] + right]
        if i:
            parts = [parts[0] + left, parts[1] + middle_extra, parts[2] + right_extra]
        squares.append(jnp.concatenate(parts, 1))
    for i in range(3):
        square_low[i * n : (i + 1) * n, :] = squares[i].astype(BF16)
    whole = frame[...]
    density = []
    for i in range(3):
        product = dot(square_low[i * n : (i + 1) * n, :], whole)
        density.append((3.0 * squares[i] - 2.0 * product).astype(BF16))
    monos = [mono[...], purified(second), purified(last)]
    for i in range(3):
        frame[i * n : (i + 1) * n, :] = density[i]
    whole = frame[...]
    results = []
    for i in range(3):
        square = dot(whole[i * n : (i + 1) * n, :], whole)
        product = dot(square.astype(BF16), whole[:, i * n : (i + 1) * n])
        results.append(3.0 * square[:, i * n : (i + 1) * n] - 2.0 * product)
    stay_code = rows[base : base + 1, :]
    leave_code = rows[base + 1 : base + 2, :]
    last_code = rows[base + 2 : base + 3, :]
    correction = results[1] - monos[1]
    pack_into(going, 0, correction, leave_code)
    pack_into(going, 1, results[2] - monos[2], last_code)
    pack_into(staying, 0, correction, stay_code)
    mine[...] = monos[0] + (results[0] - monos[0]).astype(BF16).astype(F32)


def collect_kernel(back, staying, rows, *outs, workers):
    n = back.shape[-1]
    half = n // 2
    base = 3 * workers + 2
    pieces = [(back[0], back[0, half + 1 : half + 2, :]), (back[1], back[1, half + 1 : half + 2, :])]
    pieces.append((staying[0], staying[0, half + 1 : half + 2, :]))
    pieces = [(piece.astype(F32), code.astype(F32)) for piece, code in pieces]
    for k in range(workers):
        slot = rows[base + k : base + k + 1, :]
        total = jnp.zeros((half + PAD, n), F32)
        for piece, code in pieces:
            total = total + jnp.where(code == slot, piece, 0.0)
        outs[k][0] = total.astype(BF16)


def finish_kernel(*refs):
    *packed, mine, out = refs
    n = mine.shape[-1]
    half = n // 2
    total = packed[0][0].astype(F32)
    for ref in packed[1:]:
        total = total + ref[0].astype(F32)
    parts = unpack(total[:half, :half], total[:half, half:], total[half : half + 1, :half])
    upper_left, upper_right, lower_left, lower_right = parts
    out[0, :half, :half] = mine[:half, :half] + upper_left
    out[0, :half, half:] = mine[:half, half:] + upper_right
    out[0, half:, :half] = mine[half:, :half] + lower_left
    out[0, half:, half:] = mine[half:, half:] + lower_right


def call(kernel, operands, outs, flops=0, scratch=(), scalars=False, limit=24):
    vmem = pl.BlockSpec(memory_space=pltpu.VMEM)
    specs = [vmem] * len(operands)
    if scalars:
        specs[0] = pl.BlockSpec(memory_space=pltpu.SMEM)
    return pl.pallas_call(
        kernel,
        in_specs=specs,
        out_specs=[vmem] * len(outs),
        out_shape=[jax.ShapeDtypeStruct(*out) for out in outs],
        scratch_shapes=scratch,
        cost_estimate=pl.CostEstimate(flops=flops, bytes_accessed=0, transcendentals=0),
        compiler_params=pltpu.CompilerParams(vmem_limit_bytes=limit * 1024 * 1024),
    )(*operands)


def shards(mono_ham, polymer_members, polymer_coupling):
    import functools

    workers = lax.axis_size("wrk")
    groups = lax.axis_size("grp")
    n = mono_ham.shape[-1]
    tall = n // 2 + PAD
    own_group = lax.axis_index("grp").astype(jnp.int32)
    own_slot = lax.axis_index("wrk").astype(jnp.int32)
    scalars = jnp.concatenate(
        [polymer_members[0], own_group[None], own_slot[None], jnp.full((3,), groups, jnp.int32)]
    )
    (packed,) = call(pack_kernel, (mono_ham,), [((1, tall, n), BF16)], flops=1000)
    order = sorted(range(1, workers), key=lambda k: (min(k, workers - k), k))
    mates = {k: from_behind(packed, "wrk", -k) for k in order}
    following = [from_behind(b, "grp", -1) for b in [packed] + [mates[k] for k in range(1, workers)]]
    n_rows = 4 * workers + 2
    frame, known, mono, rows = call(
        functools.partial(early_kernel, workers=workers),
        (scalars, mono_ham, polymer_coupling),
        [((3 * n, 3 * n), BF16), ((3 * n, 3 * n), F32), ((n, n), F32), ((n_rows, n), F32)],
        flops=2 * 31 * n**3,
        scalars=True,
    )
    going, staying, mine = call(
        functools.partial(main_kernel, workers=workers),
        [mates[k] for k in range(1, workers)] + following + [frame, known, mono, rows],
        [((2, tall, n), BF16), ((1, tall, n), BF16), ((n, n), F32)],
        flops=2 * 90 * n**3,
        scratch=[pltpu.VMEM((3 * n, 3 * n), BF16), pltpu.VMEM((3 * n, 3 * n), BF16)],
    )
    back = from_behind(going, "grp", 1)
    sums = call(
        functools.partial(collect_kernel, workers=workers),
        (back, staying, rows),
        [((1, tall, n), BF16)] * workers,
        flops=1000,
    )
    received = [from_behind(sums[k], "wrk", -k) for k in order]
    (density,) = call(finish_kernel, [sums[0]] + received + [mine], [((1, n, n), F32)], flops=1000)
    return density


def solution(mesh):
    placed = (
        P(("grp", "wrk"), None, None),
        P(("grp", "wrk"), None),
        P(("grp", "wrk"), None, None, None),
    )
    return jax.shard_map(
        shards, mesh=mesh, in_specs=placed, out_specs=P(("grp", "wrk"), None, None), check_vma=False
    )
```

```python
import functools

import jax
import jax.numpy as jnp
from jax import lax
from jax.experimental import pallas as pl
from jax.experimental.pallas import tpu as pltpu
from jax.sharding import PartitionSpec as P


F32 = jnp.float32
BF16 = jnp.bfloat16
PAD = 8


def from_behind(block, axis, distance):
    devices = range(lax.axis_size(axis))
    route = [((i - distance) % len(devices), i) for i in devices]
    return lax.ppermute(block, axis, route)


def dot(a, b):
    return jnp.dot(a, b, preferred_element_type=F32)


def grid_masks(half):
    row = lax.broadcasted_iota(jnp.int32, (half, half), 0)
    col = lax.broadcasted_iota(jnp.int32, (half, half), 1)
    return row, col


def eye(n):
    row, col = grid_masks(n)
    return jnp.where(row == col, 1.0, 0.0)


def pack_into(ref, index, block, code=None):
    n = block.shape[-1]
    half = n // 2
    row, col = grid_masks(half)
    low = block[half:, half:]
    folded = jnp.where(row >= col, block[:half, :half], low)
    diagonal = jnp.sum(jnp.where(row == col, low, 0.0), axis=0, keepdims=True)
    ref[index, :half, :] = folded.astype(BF16)
    ref[index, half:n, :] = block[:half, half:].astype(BF16)
    tail = jnp.broadcast_to(diagonal, (PAD, half))
    if code is not None:
        line = lax.broadcasted_iota(jnp.int32, (PAD, half), 0)
        tail = jnp.where(line == 0, tail, code)
    ref[index, n:, :] = tail.astype(BF16)


def unpack(packed):
    half = packed.shape[-1]
    folded, corner, diagonal = packed[:half], packed[half : 2 * half], packed[2 * half : 2 * half + 1]
    row, col = grid_masks(half)
    turned = folded.T
    first = jnp.where(row >= col, folded, turned)
    last = jnp.where(row < col, folded, jnp.where(row > col, turned, diagonal))
    return first, corner, corner.T, last


def purified(low):
    square = dot(low, low)
    density = 3.0 * square - 2.0 * dot(square.astype(BF16), low)
    low = density.astype(BF16)
    square = dot(low, low)
    return 3.0 * square - 2.0 * dot(square.astype(BF16), low)


def pack_kernel(ham, out, own):
    n = ham.shape[-1]
    block = 0.5 * eye(n) - 0.35 * ham[0].astype(F32)
    pack_into(out, 0, block)
    own[...] = block.astype(BF16)


def early_kernel(members, own_ref, coupling, frame, known, rows, *, workers, groups):
    n = own_ref.shape[-1]
    group = lax.axis_index("grp")
    slot = lax.axis_index("wrk")
    following = lax.rem(group + 1, groups)
    second, last = members[0, 1], members[0, 2]
    line = 0

    def put(value):
        nonlocal line
        rows[line, :] = jnp.full((n // 2,), value, F32)
        line += 1

    for k in range(1, workers):
        mate = group * workers + lax.rem(slot + k, workers)
        put(jnp.where(second == mate, 1.0, 0.0))
    for member in (second, last):
        for k in range(workers):
            mate = following * workers + lax.rem(slot + k, workers)
            put(jnp.where(member == mate, 1.0, 0.0))
    inside = (second >= group * workers) & (second < (group + 1) * workers)
    second_slot = lax.rem(second, workers).astype(F32)
    put(jnp.where(inside, second_slot, -1.0))
    put(jnp.where(inside, -1.0, second_slot))
    put(jnp.where(last >= 0, lax.rem(last, workers), -1).astype(F32))
    for k in range(workers):
        put(lax.rem(slot + workers - k, workers).astype(F32))
    own = own_ref[...]
    third = jnp.where(last >= 0, 1.0, 0.0)
    c01 = -0.35 * coupling[0, 0].astype(F32)
    c02 = -0.35 * coupling[0, 1].astype(F32) * third
    c12 = -0.35 * coupling[0, 2].astype(F32) * third
    frame[:n, :n] = own
    frame[:n, n : 2 * n] = c01.astype(BF16)
    frame[:n, 2 * n :] = c02.astype(BF16)
    frame[n : 2 * n, :n] = c01.T.astype(BF16)
    frame[n : 2 * n, n : 2 * n] = jnp.zeros((n, n), BF16)
    frame[n : 2 * n, 2 * n :] = c12.astype(BF16)
    frame[2 * n :, :n] = c02.T.astype(BF16)
    frame[2 * n :, n : 2 * n] = c12.T.astype(BF16)
    frame[2 * n :, 2 * n :] = jnp.zeros((n, n), BF16)
    for j in range(3):
        part = slice(j * n, (j + 1) * n)
        known[: (j + 1) * n, part] = dot(frame[: (j + 1) * n, :], frame[:, part])


def main_kernel(*refs, workers):
    own = refs[: workers - 1]
    following = refs[workers - 1 : 2 * workers - 1]
    first, known, rows, going, frame, crossed, low = refs[2 * workers - 1 :]
    n = known.shape[-1] // 3
    half = n // 2
    base = 3 * workers - 1

    def part(i):
        return slice(i * n, (i + 1) * n)

    def chosen(candidates, first_row):
        total = jnp.zeros((n + PAD, half), F32)
        for c, ref in enumerate(candidates):
            total = jnp.where(rows[first_row + c : first_row + c + 1, :] > 0.5, ref[0].astype(F32), total)
        return total

    members = []
    for packed in (chosen(own + following, 0), chosen(following, 2 * workers - 1)):
        a, b, c, d = unpack(packed)
        block = jnp.concatenate([jnp.concatenate([a, b], 1), jnp.concatenate([c, d], 1)], 0)
        members.append(block)
    second, last = [block.astype(BF16) for block in members]
    blocks = {(i, j): first[part(i), part(j)] for i in range(3) for j in range(3)}
    blocks[1, 1], blocks[2, 2] = second, last

    def rectangle(table, down, across):
        return jnp.concatenate([jnp.concatenate([table[i, j] for j in across], 1) for i in down], 0)

    square = {(i, j): known[part(i), part(j)] for j in range(3) for i in range(j + 1)}
    extra = dot(rectangle(blocks, (0, 1), (1,)), second)
    square[0, 1] += extra[:n]
    square[1, 1] += extra[n:]
    extra = dot(rectangle(blocks, (0, 1, 2), (2,)), last)
    square[0, 2] += extra[:n]
    square[1, 2] += extra[n : 2 * n] + dot(second, blocks[1, 2])
    square[2, 2] += extra[2 * n :]
    for (i, j), value in square.items():
        low[part(i), part(j)] = value.astype(BF16)
        if i < j:
            low[part(j), part(i)] = value.T.astype(BF16)
    for j in range(3):
        product = dot(rectangle(blocks, range(j + 1), range(3)), low[:, part(j)])
        for i in range(j + 1):
            value = 3.0 * square[i, j] - 2.0 * product[part(i)]
            frame[part(i), part(j)] = value.astype(BF16)
            if i < j:
                frame[part(j), part(i)] = value.T.astype(BF16)
    square = {}
    for j in (1, 2):
        product = dot(frame[: (j + 1) * n, :], frame[:, part(j)])
        for i in range(j + 1):
            square[i, j] = product[part(i)]
            low[part(i), part(j)] = square[i, j].astype(BF16)
            if i == 1 and j == 2:
                low[part(j), part(i)] = square[i, j].T.astype(BF16)
    crossed[0] = square[0, 1].T.astype(BF16)
    crossed[1] = square[0, 2].T.astype(BF16)
    for s in (1, 2):
        density = 3.0 * square[s, s] - 2.0 * dot(frame[part(s), :], low[:, part(s)])
        pack_into(going, s - 1, density - members[s - 1], rows[base + s : base + s + 1, :])


def own_kernel(own, frame, crossed, mine, delta):
    n = mine.shape[-1]
    delta[...] = own[...].astype(F32) - purified(own[...])
    square = dot(frame[:n, :], frame[:, :n])
    low = jnp.concatenate([square.astype(BF16), crossed[0], crossed[1]], 0)
    mine[...] = 3.0 * square - 2.0 * dot(frame[:n, :], low)


def collect_kernel(back, going, rows, *outs, workers):
    half = back.shape[-1]
    n = 2 * half
    base = 3 * workers + 2
    line = lax.broadcasted_iota(jnp.int32, (n + PAD, half), 0)
    pieces = []
    for piece in (back[0], back[1]):
        piece = piece.astype(F32)
        pieces.append((piece, piece[n + 1 : n + 2, :]))
    pieces.append((going[0].astype(F32), rows[base - 3 : base - 2, :]))
    pieces = [(jnp.where(line > n, 1.0, piece), code) for piece, code in pieces]
    for k in range(workers):
        slot = rows[base + k : base + k + 1, :]
        total = jnp.zeros((n + PAD, half), F32)
        for piece, code in pieces:
            total = total + jnp.where(code == slot, piece, 0.0)
        outs[k][0] = total.astype(BF16)


def finish_kernel(*refs):
    *packed, mine, delta, out = refs
    n = mine.shape[-1]
    half = n // 2
    total = packed[0][0].astype(F32)
    for ref in packed[1:]:
        total = total + ref[0].astype(F32)
    count = total[n + 1 : n + 2, :]
    top, bottom = slice(0, half), slice(half, n)
    for value, down, across in zip(unpack(total), (top, top, bottom, bottom), (top, bottom, top, bottom)):
        out[0, down, across] = mine[down, across] + count * delta[down, across] + value


def call(kernel, operands, outs, flops=0, scratch=(), spaces=None, limit=24):
    vmem = pl.BlockSpec(memory_space=pltpu.VMEM)
    specs = [vmem] * len(operands)
    for at, space in (spaces or {}).items():
        specs[at] = pl.BlockSpec(memory_space=space)
    return pl.pallas_call(
        kernel,
        in_specs=specs,
        out_specs=[vmem] * len(outs),
        out_shape=[jax.ShapeDtypeStruct(*out) for out in outs],
        scratch_shapes=scratch,
        cost_estimate=pl.CostEstimate(flops=flops, bytes_accessed=0, transcendentals=0),
        compiler_params=pltpu.CompilerParams(vmem_limit_bytes=limit * 1024 * 1024),
    )(*operands)


def in_order(workers):
    return list(range(workers - 1, 0, -1))


def out_order(workers):
    return list(range(workers - 1, 0, -1))


def step(mono_ham, polymer_members, polymer_coupling):
    workers = lax.axis_size("wrk")
    groups = lax.axis_size("grp")
    n = mono_ham.shape[-1]
    tall, wide = n + PAD, n // 2
    packed, own = call(pack_kernel, (mono_ham,), [((1, tall, wide), BF16), ((n, n), BF16)], flops=1000)
    mates = {}
    for k in in_order(workers):
        mates[k] = from_behind(packed, "wrk", -k)
    following = []
    for k in range(workers):
        following.append(from_behind(mates[k] if k else packed, "grp", -1))
    n_rows = 4 * workers + 2
    frame, known, rows = call(
        functools.partial(early_kernel, workers=workers, groups=groups),
        (polymer_members, own, polymer_coupling),
        [((3 * n, 3 * n), BF16), ((3 * n, 3 * n), F32), ((n_rows, wide), F32)],
        flops=2 * 18 * n**3,
        spaces={0: pltpu.SMEM},
    )
    going, frame, crossed = call(
        functools.partial(main_kernel, workers=workers),
        [mates[k] for k in range(1, workers)] + following + [frame, known, rows],
        [((2, tall, wide), BF16), ((3 * n, 3 * n), BF16), ((2, n, n), BF16)],
        flops=2 * 45 * n**3,
        scratch=[pltpu.VMEM((3 * n, 3 * n), BF16)],
    )
    back = from_behind(going, "grp", 1)
    mine, delta = call(own_kernel, (own, frame, crossed), [((n, n), F32)] * 2, flops=2 * 10 * n**3)
    sums = call(
        functools.partial(collect_kernel, workers=workers),
        (back, going, rows),
        [((1, tall, wide), BF16)] * workers,
        flops=1000,
    )
    received = []
    for k in out_order(workers):
        received.append(from_behind(sums[k], "wrk", -k))
    (density,) = call(finish_kernel, [sums[0]] + received + [mine, delta], [((1, n, n), F32)], flops=1000)
    return density


def solution(mesh):
    placed = (
        P(("grp", "wrk"), None, None),
        P(("grp", "wrk"), None),
        P(("grp", "wrk"), None, None, None),
    )
    return jax.shard_map(step, mesh=mesh, in_specs=placed, out_specs=P(("grp", "wrk"), None, None), check_vma=False)
```

```python
import functools

import jax
import jax.numpy as jnp
from jax import lax
from jax.experimental import pallas as pl
from jax.experimental.pallas import tpu as pltpu
from jax.sharding import PartitionSpec as P


F32 = jnp.float32
BF16 = jnp.bfloat16
PAD = 8


def mate(slot, k, workers):
    return slot ^ k if workers == 4 else lax.rem(slot + k, workers)


def pairs(distance, k):
    groups, workers = lax.axis_size("grp"), lax.axis_size("wrk")
    for g in range(groups):
        for w in range(workers):
            other = w ^ k if workers == 4 else (w + k) % workers
            yield g * workers + w, (g + distance) % groups * workers + other


def from_mate(block, distance, k):
    return lax.ppermute(block, ("grp", "wrk"), [(there, here) for here, there in pairs(distance, k)])


def to_mate(block, distance, k):
    return lax.ppermute(block, ("grp", "wrk"), list(pairs(distance, k)))


def everyone(workers):
    return [(0, k) for k in range(1, workers)] + [(1, k) for k in range(workers)]


def gather_plan(workers):
    if workers == 4:
        return [(0, 2, None), (1, 1, None), (0, 1, None), (1, 0, None), (0, 1, 2), (1, 1, 2), (1, 0, 2)]
    return [(distance, k, None) for distance, k in everyone(workers)]


def gather(packed):
    blocks = {}
    for distance, k, what in gather_plan(lax.axis_size("wrk")):
        sent = packed if what is None else blocks[0, what]
        blocks[distance, k ^ (what or 0)] = from_mate(sent, distance, k)
    return [blocks[at] for at in everyone(lax.axis_size("wrk"))]


def return_plan(workers):
    if workers == 4:
        return [(1, 1, 3), (1, 0, 2), (0, 1, 3), (1, 0, 0), (1, 1, 1), (0, 1, 1)]
    return [(distance, k, k) for distance, k in everyone(workers)]


def give_back(pieces):
    workers = lax.axis_size("wrk")
    near, far = [], []
    for distance, k, owner in return_plan(workers):
        block = to_mate(pieces[distance, owner], distance, k)
        (near if k == owner else far).append(block)
    if far:
        (total,) = call(add_kernel, far + [pieces[0, 2]], [(far[0].shape, BF16)], flops=1000)
        near.append(to_mate(total, 0, 2))
    return near


def dot(a, b):
    return jnp.dot(a, b, preferred_element_type=F32)


def grid_masks(half):
    row = lax.broadcasted_iota(jnp.int32, (half, half), 0)
    col = lax.broadcasted_iota(jnp.int32, (half, half), 1)
    return row, col


def eye(n):
    row, col = grid_masks(n)
    return jnp.where(row == col, 1.0, 0.0)


def pack(block):
    n = block.shape[-1]
    half = n // 2
    row, col = grid_masks(half)
    low = block[half:, half:]
    folded = jnp.where(row >= col, block[:half, :half], low)
    diagonal = jnp.sum(jnp.where(row == col, low, 0.0), axis=0, keepdims=True)
    line = lax.broadcasted_iota(jnp.int32, (PAD, half), 0)
    tail = jnp.where(line == 0, diagonal, 1.0)
    return jnp.concatenate([folded, block[:half, half:], tail], 0)


def unpack(packed):
    half = packed.shape[-1]
    folded, corner, diagonal = packed[:half], packed[half : 2 * half], packed[2 * half : 2 * half + 1]
    row, col = grid_masks(half)
    turned = folded.T
    first = jnp.where(row >= col, folded, turned)
    last = jnp.where(row < col, folded, jnp.where(row > col, turned, diagonal))
    return first, corner, corner.T, last


def purified(low):
    square = dot(low, low)
    density = 3.0 * square - 2.0 * dot(square.astype(BF16), low)
    low = density.astype(BF16)
    square = dot(low, low)
    return 3.0 * square - 2.0 * dot(square.astype(BF16), low)


def pack_kernel(ham, out, own):
    n = ham.shape[-1]
    block = 0.5 * eye(n) - 0.35 * ham[0].astype(F32)
    out[0] = pack(block).astype(BF16)
    own[...] = block.astype(BF16)


def early_kernel(members, own_ref, coupling, frame, known, rows, *, workers, groups):
    n = own_ref.shape[-1]
    group = lax.axis_index("grp")
    slot = lax.axis_index("wrk")
    following = lax.rem(group + 1, groups)
    second, last = members[:, 1:2], members[:, 2:3]
    line = 0

    def put(value):
        nonlocal line
        rows[line : line + 1, :] = jnp.broadcast_to(value, (1, n // 2)).astype(F32)
        line += 1

    def hit(member, member_group, member_slot):
        return jnp.where(member == member_group * workers + member_slot, 1.0, 0.0)

    for k in range(1, workers):
        put(hit(second, group, mate(slot, k, workers)))
    for member in (second, last):
        for k in range(workers):
            put(hit(member, following, mate(slot, k, workers)))
    own = own_ref[...]
    third = jnp.where(last >= 0, 1.0, 0.0)
    c01 = -0.35 * coupling[0, 0].astype(F32)
    c02 = -0.35 * coupling[0, 1].astype(F32) * third
    c12 = -0.35 * coupling[0, 2].astype(F32) * third
    frame[:n, :n] = own
    frame[:n, n : 2 * n] = c01.astype(BF16)
    frame[:n, 2 * n :] = c02.astype(BF16)
    frame[n : 2 * n, :n] = c01.T.astype(BF16)
    frame[n : 2 * n, n : 2 * n] = jnp.zeros((n, n), BF16)
    frame[n : 2 * n, 2 * n :] = c12.astype(BF16)
    frame[2 * n :, :n] = c02.T.astype(BF16)
    frame[2 * n :, n : 2 * n] = c12.T.astype(BF16)
    frame[2 * n :, 2 * n :] = jnp.zeros((n, n), BF16)
    for j in range(3):
        part = slice(j * n, (j + 1) * n)
        known[: (j + 1) * n, part] = dot(frame[: (j + 1) * n, :], frame[:, part])


def main_kernel(*refs, workers):
    own = refs[: workers - 1]
    following = refs[workers - 1 : 2 * workers - 1]
    first, known, rows = refs[2 * workers - 1 : 2 * workers + 2]
    sent = refs[2 * workers + 2 : -3]
    frame, crossed, low = refs[-3:]
    n = known.shape[-1] // 3
    half = n // 2

    def part(i):
        return slice(i * n, (i + 1) * n)

    def chosen(candidates, first_row):
        total = jnp.zeros((n + PAD, half), F32)
        for c, ref in enumerate(candidates):
            total = jnp.where(rows[first_row + c : first_row + c + 1, :] > 0.5, ref[0].astype(F32), total)
        return total

    members = []
    for packed in (chosen(own + following, 0), chosen(following, 2 * workers - 1)):
        a, b, c, d = unpack(packed)
        block = jnp.concatenate([jnp.concatenate([a, b], 1), jnp.concatenate([c, d], 1)], 0)
        members.append(block)
    second, last = [block.astype(BF16) for block in members]
    blocks = {(i, j): first[part(i), part(j)] for i in range(3) for j in range(3)}
    blocks[1, 1], blocks[2, 2] = second, last

    def rectangle(table, down, across):
        return jnp.concatenate([jnp.concatenate([table[i, j] for j in across], 1) for i in down], 0)

    square = {(i, j): known[part(i), part(j)] for j in range(3) for i in range(j + 1)}
    extra = dot(rectangle(blocks, (0, 1), (1,)), second)
    square[0, 1] += extra[:n]
    square[1, 1] += extra[n:]
    extra = dot(rectangle(blocks, (0, 1, 2), (2,)), last)
    square[0, 2] += extra[:n]
    square[1, 2] += extra[n : 2 * n] + dot(second, blocks[1, 2])
    square[2, 2] += extra[2 * n :]
    for (i, j), value in square.items():
        low[part(i), part(j)] = value.astype(BF16)
        if i < j:
            low[part(j), part(i)] = value.T.astype(BF16)
    for j in range(3):
        product = dot(rectangle(blocks, range(j + 1), range(3)), low[:, part(j)])
        for i in range(j + 1):
            value = 3.0 * square[i, j] - 2.0 * product[part(i)]
            frame[part(i), part(j)] = value.astype(BF16)
            if i < j:
                frame[part(j), part(i)] = value.T.astype(BF16)
    square = {}
    for j in (1, 2):
        product = dot(frame[: (j + 1) * n, :], frame[:, part(j)])
        for i in range(j + 1):
            square[i, j] = product[part(i)]
            low[part(i), part(j)] = square[i, j].astype(BF16)
            if i == 1 and j == 2:
                low[part(j), part(i)] = square[i, j].T.astype(BF16)
    crossed[0] = square[0, 1].T.astype(BF16)
    crossed[1] = square[0, 2].T.astype(BF16)
    pieces = []
    for s in (1, 2):
        density = 3.0 * square[s, s] - 2.0 * dot(frame[part(s), :], low[:, part(s)])
        pieces.append(pack(density - members[s - 1]))
    for at, ref in enumerate(sent):
        value = jnp.where(rows[at : at + 1, :] > 0.5, pieces[0], 0.0)
        if at >= workers - 1:
            value = jnp.where(rows[at + workers : at + workers + 1, :] > 0.5, pieces[1], value)
        ref[0] = value.astype(BF16)


def own_kernel(own, frame, crossed, mine, delta):
    n = mine.shape[-1]
    delta[...] = own[...].astype(F32) - purified(own[...])
    square = dot(frame[:n, :], frame[:, :n])
    low = jnp.concatenate([square.astype(BF16), crossed[0], crossed[1]], 0)
    mine[...] = 3.0 * square - 2.0 * dot(frame[:n, :], low)


def add_kernel(*refs):
    *parts, out = refs
    total = parts[0][...].astype(F32)
    for ref in parts[1:]:
        total = total + ref[...].astype(F32)
    out[...] = total.astype(BF16)


def finish_kernel(*refs):
    *packed, mine, delta, out = refs
    n = mine.shape[-1]
    half = n // 2
    total = packed[0][0].astype(F32)
    for ref in packed[1:]:
        total = total + ref[0].astype(F32)
    count = total[n + 1 : n + 2, :]
    top, bottom = slice(0, half), slice(half, n)
    for value, down, across in zip(unpack(total), (top, top, bottom, bottom), (top, bottom, top, bottom)):
        out[0, down, across] = mine[down, across] + count * delta[down, across] + value


def call(kernel, operands, outs, flops=0, scratch=(), limit=24):
    vmem = pl.BlockSpec(memory_space=pltpu.VMEM)
    return pl.pallas_call(
        kernel,
        in_specs=[vmem] * len(operands),
        out_specs=[vmem] * len(outs),
        out_shape=[jax.ShapeDtypeStruct(*out) for out in outs],
        scratch_shapes=scratch,
        cost_estimate=pl.CostEstimate(flops=flops, bytes_accessed=0, transcendentals=0),
        compiler_params=pltpu.CompilerParams(vmem_limit_bytes=limit * 1024 * 1024),
    )(*operands)


def step(mono_ham, polymer_members, polymer_coupling):
    workers = lax.axis_size("wrk")
    groups = lax.axis_size("grp")
    n = mono_ham.shape[-1]
    tall, wide = n + PAD, n // 2
    packed, own = call(pack_kernel, (mono_ham,), [((1, tall, wide), BF16), ((n, n), BF16)], flops=1000)
    candidates = gather(packed)
    frame, known, rows = call(
        functools.partial(early_kernel, workers=workers, groups=groups),
        (polymer_members, own, polymer_coupling),
        [((3 * n, 3 * n), BF16), ((3 * n, 3 * n), F32), ((3 * workers - 1, wide), F32)],
        flops=2 * 18 * n**3,
    )
    targets = everyone(workers)
    *sent, frame, crossed = call(
        functools.partial(main_kernel, workers=workers),
        candidates + [frame, known, rows],
        [((1, tall, wide), BF16)] * len(targets) + [((3 * n, 3 * n), BF16), ((2, n, n), BF16)],
        flops=2 * 45 * n**3,
        scratch=[pltpu.VMEM((3 * n, 3 * n), BF16)],
    )
    received = give_back(dict(zip(targets, sent)))
    mine, delta = call(own_kernel, (own, frame, crossed), [((n, n), F32)] * 2, flops=2 * 10 * n**3)
    (density,) = call(finish_kernel, received + [mine, delta], [((1, n, n), F32)], flops=1000)
    return density


def solution(mesh):
    placed = (
        P(("grp", "wrk"), None, None),
        P(("grp", "wrk"), None),
        P(("grp", "wrk"), None, None, None),
    )
    return jax.shard_map(step, mesh=mesh, in_specs=placed, out_specs=P(("grp", "wrk"), None, None), check_vma=False)
```

```python
import functools

import jax
import jax.numpy as jnp
from jax import lax
from jax.experimental import pallas as pl
from jax.experimental.pallas import tpu as pltpu
from jax.sharding import PartitionSpec as P


F32 = jnp.float32
BF16 = jnp.bfloat16
PAD = 8


def mate(slot, k, workers):
    return slot ^ k if workers == 4 else lax.rem(slot + k, workers)


def pairs(distance, k):
    groups, workers = lax.axis_size("grp"), lax.axis_size("wrk")
    for g in range(groups):
        for w in range(workers):
            other = w ^ k if workers == 4 else (w + k) % workers
            yield g * workers + w, (g + distance) % groups * workers + other


def from_mate(block, distance, k):
    return lax.ppermute(block, ("grp", "wrk"), [(there, here) for here, there in pairs(distance, k)])


def to_mate(block, distance, k):
    return lax.ppermute(block, ("grp", "wrk"), list(pairs(distance, k)))


def everyone(workers):
    return [(0, k) for k in range(1, workers)] + [(1, k) for k in range(workers)]


def gather_plan(workers):
    if workers == 4:
        return [(0, 2, None), (0, 1, None), (1, 1, None), (1, 0, None), (0, 1, 2), (1, 0, 2), (1, 1, 2)]
    return [(distance, k, None) for distance, k in everyone(workers)]


def gather(packed):
    blocks = {}
    for distance, k, what in gather_plan(lax.axis_size("wrk")):
        sent = packed if what is None else blocks[0, what]
        blocks[distance, k ^ (what or 0)] = from_mate(sent, distance, k)
    return [blocks[at] for at in everyone(lax.axis_size("wrk"))]


def return_plan(workers):
    if workers == 4:
        return [(1, 1, 3), (1, 0, 2), (0, 1, 3), (1, 0, 0), (1, 1, 1), (0, 1, 1)]
    return [(distance, k, k) for distance, k in everyone(workers)]


def give_back(pieces):
    workers = lax.axis_size("wrk")
    near, far = [], []
    for distance, k, owner in return_plan(workers):
        block = to_mate(pieces[distance, owner], distance, k)
        (near if k == owner else far).append(block)
    if far:
        (total,) = call(add_kernel, far + [pieces[0, 2]], [(far[0].shape, BF16)], flops=1000)
        near.append(to_mate(total, 0, 2))
    return near


def dot(a, b):
    return jnp.dot(a, b, preferred_element_type=F32)


def grid_masks(half):
    row = lax.broadcasted_iota(jnp.int32, (half, half), 0)
    col = lax.broadcasted_iota(jnp.int32, (half, half), 1)
    return row, col


def eye(n):
    row, col = grid_masks(n)
    return jnp.where(row == col, 1.0, 0.0)


def pack(block):
    n = block.shape[-1]
    half = n // 2
    row, col = grid_masks(half)
    low = block[half:, half:]
    folded = jnp.where(row >= col, block[:half, :half], low)
    diagonal = jnp.sum(jnp.where(row == col, low, 0.0), axis=0, keepdims=True)
    line = lax.broadcasted_iota(jnp.int32, (PAD, half), 0)
    tail = jnp.where(line == 0, diagonal, 1.0)
    return jnp.concatenate([folded, block[:half, half:], tail], 0)


def unpack(packed):
    half = packed.shape[-1]
    folded, corner, diagonal = packed[:half], packed[half : 2 * half], packed[2 * half : 2 * half + 1]
    row, col = grid_masks(half)
    turned = folded.T
    first = jnp.where(row >= col, folded, turned)
    last = jnp.where(row < col, folded, jnp.where(row > col, turned, diagonal))
    return first, corner, corner.T, last


def purified(low):
    square = dot(low, low)
    density = 3.0 * square - 2.0 * dot(square.astype(BF16), low)
    low = density.astype(BF16)
    square = dot(low, low)
    return 3.0 * square - 2.0 * dot(square.astype(BF16), low)


def pack_kernel(ham, out, own):
    n = ham.shape[-1]
    block = 0.5 * eye(n) - 0.35 * ham[0].astype(F32)
    out[0] = pack(block).astype(BF16)
    own[...] = block.astype(BF16)


def early_kernel(
    members_hbm, coupling_hbm, own_ref, frame, known, rows, members, coupling, arrived, *, workers, groups
):
    n = own_ref.shape[-1]
    listing = pltpu.make_async_copy(members_hbm, members, arrived.at[0])
    fetch = pltpu.make_async_copy(coupling_hbm, coupling, arrived.at[1])
    listing.start()
    fetch.start()
    listing.wait()
    group = lax.axis_index("grp")
    slot = lax.axis_index("wrk")
    following = lax.rem(group + 1, groups)
    second, last = members[:, 1:2], members[:, 2:3]
    line = 0

    def put(value):
        nonlocal line
        rows[line : line + 1, :] = jnp.broadcast_to(value, (1, n // 2)).astype(F32)
        line += 1

    def hit(member, member_group, member_slot):
        return jnp.where(member == member_group * workers + member_slot, 1.0, 0.0)

    for k in range(1, workers):
        put(hit(second, group, mate(slot, k, workers)))
    for member in (second, last):
        for k in range(workers):
            put(hit(member, following, mate(slot, k, workers)))
    own = own_ref[...]
    third = jnp.where(last >= 0, 1.0, 0.0)
    fetch.wait()
    c01 = -0.35 * coupling[0, 0].astype(F32)
    c02 = -0.35 * coupling[0, 1].astype(F32) * third
    c12 = -0.35 * coupling[0, 2].astype(F32) * third
    frame[:n, :n] = own
    frame[:n, n : 2 * n] = c01.astype(BF16)
    frame[:n, 2 * n :] = c02.astype(BF16)
    frame[n : 2 * n, :n] = c01.T.astype(BF16)
    frame[n : 2 * n, n : 2 * n] = jnp.zeros((n, n), BF16)
    frame[n : 2 * n, 2 * n :] = c12.astype(BF16)
    frame[2 * n :, :n] = c02.T.astype(BF16)
    frame[2 * n :, n : 2 * n] = c12.T.astype(BF16)
    frame[2 * n :, 2 * n :] = jnp.zeros((n, n), BF16)
    for j in range(3):
        part = slice(j * n, (j + 1) * n)
        known[: (j + 1) * n, part] = dot(frame[: (j + 1) * n, :], frame[:, part])


def main_kernel(*refs, workers):
    own = refs[: workers - 1]
    following = refs[workers - 1 : 2 * workers - 1]
    first, known, rows = refs[2 * workers - 1 : 2 * workers + 2]
    sent = refs[2 * workers + 2 : -3]
    frame, crossed, low = refs[-3:]
    n = known.shape[-1] // 3
    half = n // 2

    def part(i):
        return slice(i * n, (i + 1) * n)

    def chosen(candidates, first_row):
        total = jnp.zeros((n + PAD, half), F32)
        for c, ref in enumerate(candidates):
            total = jnp.where(rows[first_row + c : first_row + c + 1, :] > 0.5, ref[0].astype(F32), total)
        return total

    members = []
    for packed in (chosen(own + following, 0), chosen(following, 2 * workers - 1)):
        a, b, c, d = unpack(packed)
        block = jnp.concatenate([jnp.concatenate([a, b], 1), jnp.concatenate([c, d], 1)], 0)
        members.append(block)
    second, last = [block.astype(BF16) for block in members]
    blocks = {(i, j): first[part(i), part(j)] for i in range(3) for j in range(3)}
    blocks[1, 1], blocks[2, 2] = second, last

    def rectangle(table, down, across):
        return jnp.concatenate([jnp.concatenate([table[i, j] for j in across], 1) for i in down], 0)

    square = {(i, j): known[part(i), part(j)] for j in range(3) for i in range(j + 1)}
    extra = dot(rectangle(blocks, (0, 1), (1,)), second)
    square[0, 1] += extra[:n]
    square[1, 1] += extra[n:]
    extra = dot(rectangle(blocks, (0, 1, 2), (2,)), last)
    square[0, 2] += extra[:n]
    square[1, 2] += extra[n : 2 * n] + dot(second, blocks[1, 2])
    square[2, 2] += extra[2 * n :]
    for (i, j), value in square.items():
        low[part(i), part(j)] = value.astype(BF16)
        if i < j:
            low[part(j), part(i)] = value.T.astype(BF16)
    products = {}

    def multiply(table, down, across):
        product = dot(rectangle(table, down, range(3)), low[:, across[0] * n : (across[-1] + 1) * n])
        for a, i in enumerate(down):
            for b, j in enumerate(across):
                products[i, j] = product[part(a), part(b)]

    multiply(blocks, (0, 1), (1, 2))
    multiply(blocks, (2,), (2,))
    multiply(blocks, (0,), (0,))
    for i, j in ((0, 2), (1, 2), (2, 2), (0, 1), (1, 1), (0, 0)):
        value = 3.0 * square[i, j] - 2.0 * products[i, j]
        frame[part(i), part(j)] = value.astype(BF16)
        if i < j:
            frame[part(j), part(i)] = value.T.astype(BF16)
    product = dot(frame[: 2 * n, :], frame[:, n:])
    square = {(i, j): product[part(i), part(j - 1)] for i in (0, 1) for j in (1, 2)}
    square[2, 2] = dot(frame[2 * n :, :], frame[:, 2 * n :])
    for (i, j), value in square.items():
        low[part(i), part(j)] = value.astype(BF16)
    low[part(2), part(1)] = square[1, 2].T.astype(BF16)
    crossed[0] = square[0, 1].T.astype(BF16)
    crossed[1] = square[0, 2].T.astype(BF16)
    pieces = []
    for s in (1, 2):
        density = 3.0 * square[s, s] - 2.0 * dot(frame[part(s), :], low[:, part(s)])
        pieces.append(pack(density - members[s - 1]))
    for at, ref in enumerate(sent):
        value = jnp.where(rows[at : at + 1, :] > 0.5, pieces[0], 0.0)
        if at >= workers - 1:
            value = jnp.where(rows[at + workers : at + workers + 1, :] > 0.5, pieces[1], value)
        ref[0] = value.astype(BF16)


def own_kernel(own, frame, crossed, mine, delta):
    n = mine.shape[-1]
    delta[...] = own[...].astype(F32) - purified(own[...])
    square = dot(frame[:n, :], frame[:, :n])
    low = jnp.concatenate([square.astype(BF16), crossed[0], crossed[1]], 0)
    mine[...] = 3.0 * square - 2.0 * dot(frame[:n, :], low)


def add_kernel(*refs):
    *parts, out = refs
    total = parts[0][...].astype(F32)
    for ref in parts[1:]:
        total = total + ref[...].astype(F32)
    out[...] = total.astype(BF16)


def finish_kernel(*refs):
    *packed, mine, delta, out = refs
    n = mine.shape[-1]
    half = n // 2
    total = packed[0][0].astype(F32)
    for ref in packed[1:]:
        total = total + ref[0].astype(F32)
    count = total[n + 1 : n + 2, :]
    top, bottom = slice(0, half), slice(half, n)
    for value, down, across in zip(unpack(total), (top, top, bottom, bottom), (top, bottom, top, bottom)):
        out[0, down, across] = mine[down, across] + count * delta[down, across] + value


def in_hbm(array):
    return pltpu.with_memory_space_constraint(array, pltpu.HBM)


def call(kernel, operands, outs, flops=0, scratch=(), distant=0, limit=24):
    vmem = pl.BlockSpec(memory_space=pltpu.VMEM)
    return pl.pallas_call(
        kernel,
        in_specs=[pl.BlockSpec(memory_space=pltpu.HBM)] * distant + [vmem] * (len(operands) - distant),
        out_specs=[vmem] * len(outs),
        out_shape=[jax.ShapeDtypeStruct(*out) for out in outs],
        scratch_shapes=scratch,
        cost_estimate=pl.CostEstimate(flops=flops, bytes_accessed=0, transcendentals=0),
        compiler_params=pltpu.CompilerParams(vmem_limit_bytes=limit * 1024 * 1024),
    )(*operands)


def step(mono_ham, polymer_members, polymer_coupling):
    workers = lax.axis_size("wrk")
    groups = lax.axis_size("grp")
    n = mono_ham.shape[-1]
    tall, wide = n + PAD, n // 2
    packed, own = call(pack_kernel, (mono_ham,), [((1, tall, wide), BF16), ((n, n), BF16)], flops=1000)
    candidates = gather(packed)
    frame, known, rows = call(
        functools.partial(early_kernel, workers=workers, groups=groups),
        (in_hbm(polymer_members), in_hbm(polymer_coupling), own),
        [((3 * n, 3 * n), BF16), ((3 * n, 3 * n), F32), ((3 * workers - 1, wide), F32)],
        flops=2 * 18 * n**3,
        distant=2,
        scratch=[
            pltpu.VMEM(polymer_members.shape, jnp.int32),
            pltpu.VMEM(polymer_coupling.shape, BF16),
            pltpu.SemaphoreType.DMA((2,)),
        ],
    )
    targets = everyone(workers)
    *sent, frame, crossed = call(
        functools.partial(main_kernel, workers=workers),
        candidates + [frame, known, rows],
        [((1, tall, wide), BF16)] * len(targets) + [((3 * n, 3 * n), BF16), ((2, n, n), BF16)],
        flops=2 * 45 * n**3,
        scratch=[pltpu.VMEM((3 * n, 3 * n), BF16)],
    )
    received = give_back(dict(zip(targets, sent)))
    mine, delta = call(own_kernel, (own, frame, crossed), [((n, n), F32)] * 2, flops=2 * 10 * n**3)
    (density,) = call(finish_kernel, received + [mine, delta], [((1, n, n), F32)], flops=1000)
    return density


def solution(mesh):
    placed = (
        P(("grp", "wrk"), None, None),
        P(("grp", "wrk"), None),
        P(("grp", "wrk"), None, None, None),
    )
    return jax.shard_map(step, mesh=mesh, in_specs=placed, out_specs=P(("grp", "wrk"), None, None), check_vma=False)
```

```python
import functools

import jax
import jax.numpy as jnp
from jax import lax
from jax.experimental import pallas as pl
from jax.experimental.pallas import tpu as pltpu
from jax.sharding import PartitionSpec as P


F32 = jnp.float32
BF16 = jnp.bfloat16
PAD = 8


def mate(slot, k, workers):
    return slot ^ k if workers == 4 else lax.rem(slot + k, workers)


def pairs(distance, k):
    groups, workers = lax.axis_size("grp"), lax.axis_size("wrk")
    for g in range(groups):
        for w in range(workers):
            other = w ^ k if workers == 4 else (w + k) % workers
            yield g * workers + w, (g + distance) % groups * workers + other


def from_mate(block, distance, k):
    return lax.ppermute(block, ("grp", "wrk"), [(there, here) for here, there in pairs(distance, k)])


def to_mate(block, distance, k):
    return lax.ppermute(block, ("grp", "wrk"), list(pairs(distance, k)))


def everyone(workers):
    return [(0, k) for k in range(1, workers)] + [(1, k) for k in range(workers)]


def gather_plan(workers):
    if workers == 4:
        return [(0, 2, None), (0, 1, None), (1, 0, None), (0, 3, None), (1, 1, None), (1, 1, 2), (1, 0, 2)]
    return [(distance, k, None) for distance, k in everyone(workers)]


def gather(packed):
    blocks = {}
    for distance, k, what in gather_plan(lax.axis_size("wrk")):
        sent = packed if what is None else blocks[0, what]
        blocks[distance, k ^ (what or 0)] = from_mate(sent, distance, k)
    return [blocks[at] for at in everyone(lax.axis_size("wrk"))]


def return_plan(workers):
    if workers == 4:
        return [(1, 1, 3), (1, 0, 2), (0, 1, 3), (1, 0, 0), (1, 1, 1), (0, 1, 1)]
    return [(distance, k, k) for distance, k in everyone(workers)]


def give_back(pieces):
    workers = lax.axis_size("wrk")
    near, far = [], []
    for distance, k, owner in return_plan(workers):
        block = to_mate(pieces[distance, owner], distance, k)
        (near if k == owner else far).append(block)
    if far:
        (total,) = call(add_kernel, far + [pieces[0, 2]], [(far[0].shape, BF16)], flops=1000)
        near.append(to_mate(total, 0, 2))
    return near


def dot(a, b):
    return jnp.dot(a, b, preferred_element_type=F32)


def grid_masks(half):
    row = lax.broadcasted_iota(jnp.int32, (half, half), 0)
    col = lax.broadcasted_iota(jnp.int32, (half, half), 1)
    return row, col


def eye(n):
    row, col = grid_masks(n)
    return jnp.where(row == col, 1.0, 0.0)


def pack(block):
    n = block.shape[-1]
    half = n // 2
    row, col = grid_masks(half)
    low = block[half:, half:]
    folded = jnp.where(row >= col, block[:half, :half], low)
    diagonal = jnp.sum(jnp.where(row == col, low, 0.0), axis=0, keepdims=True)
    line = lax.broadcasted_iota(jnp.int32, (PAD, half), 0)
    tail = jnp.where(line == 0, diagonal, 1.0)
    return jnp.concatenate([folded, block[:half, half:], tail], 0)


def unpack(packed):
    half = packed.shape[-1]
    folded, corner, diagonal = packed[:half], packed[half : 2 * half], packed[2 * half : 2 * half + 1]
    row, col = grid_masks(half)
    turned = folded.T
    first = jnp.where(row >= col, folded, turned)
    last = jnp.where(row < col, folded, jnp.where(row > col, turned, diagonal))
    return first, corner, corner.T, last


def purified(low):
    square = dot(low, low)
    density = 3.0 * square - 2.0 * dot(square.astype(BF16), low)
    low = density.astype(BF16)
    square = dot(low, low)
    return 3.0 * square - 2.0 * dot(square.astype(BF16), low)


def pack_kernel(ham, out, own):
    n = ham.shape[-1]
    block = 0.5 * eye(n) - 0.35 * ham[0].astype(F32)
    out[0] = pack(block).astype(BF16)
    own[...] = block.astype(BF16)


def early_kernel(
    members_hbm, coupling_hbm, own_ref, frame, known, rows, members, coupling, arrived, *, workers, groups
):
    n = own_ref.shape[-1]
    listing = pltpu.make_async_copy(members_hbm, members, arrived.at[0])
    fetch = pltpu.make_async_copy(coupling_hbm, coupling, arrived.at[1])
    listing.start()
    fetch.start()
    listing.wait()
    group = lax.axis_index("grp")
    slot = lax.axis_index("wrk")
    following = lax.rem(group + 1, groups)
    second, last = members[:, 1:2], members[:, 2:3]
    line = 0

    def put(value):
        nonlocal line
        rows[line : line + 1, :] = jnp.broadcast_to(value, (1, n // 2)).astype(F32)
        line += 1

    def hit(member, member_group, member_slot):
        return jnp.where(member == member_group * workers + member_slot, 1.0, 0.0)

    for k in range(1, workers):
        put(hit(second, group, mate(slot, k, workers)))
    for member in (second, last):
        for k in range(workers):
            put(hit(member, following, mate(slot, k, workers)))
    own = own_ref[...]
    third = jnp.where(last >= 0, 1.0, 0.0)
    fetch.wait()
    c01 = -0.35 * coupling[0, 0].astype(F32)
    c02 = -0.35 * coupling[0, 1].astype(F32) * third
    c12 = -0.35 * coupling[0, 2].astype(F32) * third
    frame[:n, :n] = own
    frame[:n, n : 2 * n] = c01.astype(BF16)
    frame[:n, 2 * n :] = c02.astype(BF16)
    frame[n : 2 * n, :n] = c01.T.astype(BF16)
    frame[n : 2 * n, n : 2 * n] = jnp.zeros((n, n), BF16)
    frame[n : 2 * n, 2 * n :] = c12.astype(BF16)
    frame[2 * n :, :n] = c02.T.astype(BF16)
    frame[2 * n :, n : 2 * n] = c12.T.astype(BF16)
    frame[2 * n :, 2 * n :] = jnp.zeros((n, n), BF16)
    for j in range(3):
        part = slice(j * n, (j + 1) * n)
        known[: (j + 1) * n, part] = dot(frame[: (j + 1) * n, :], frame[:, part])


def main_kernel(*refs, workers):
    own = refs[: workers - 1]
    following = refs[workers - 1 : 2 * workers - 1]
    first, known, rows = refs[2 * workers - 1 : 2 * workers + 2]
    sent = refs[2 * workers + 2 : -3]
    frame, crossed, low = refs[-3:]
    n = known.shape[-1] // 3
    half = n // 2

    def part(i):
        return slice(i * n, (i + 1) * n)

    def chosen(candidates, first_row):
        total = jnp.zeros((n + PAD, half), BF16)
        for c, ref in enumerate(candidates):
            total = total + ref[0] * rows[first_row + c : first_row + c + 1, :].astype(BF16)
        return total.astype(F32)

    members = []
    for packed in (chosen(own + following, 0), chosen(following, 2 * workers - 1)):
        a, b, c, d = unpack(packed)
        block = jnp.concatenate([jnp.concatenate([a, b], 1), jnp.concatenate([c, d], 1)], 0)
        members.append(block)
    second, last = [block.astype(BF16) for block in members]
    blocks = {(i, j): first[part(i), part(j)] for i in range(3) for j in range(3)}
    blocks[1, 1], blocks[2, 2] = second, last

    def rectangle(table, down, across):
        return jnp.concatenate([jnp.concatenate([table[i, j] for j in across], 1) for i in down], 0)

    square = {(i, j): known[part(i), part(j)] for j in range(3) for i in range(j + 1)}
    extra = dot(rectangle(blocks, (0, 1), (1,)), second)
    square[0, 1] += extra[:n]
    square[1, 1] += extra[n:]
    extra = dot(rectangle(blocks, (0, 1, 2), (2,)), last)
    square[0, 2] += extra[:n]
    square[1, 2] += extra[n : 2 * n] + dot(second, blocks[1, 2])
    square[2, 2] += extra[2 * n :]
    for (i, j), value in square.items():
        low[part(i), part(j)] = value.astype(BF16)
        if i < j:
            low[part(j), part(i)] = value.astype(BF16).T
    products = {}

    def multiply(table, down, across):
        product = dot(rectangle(table, down, range(3)), low[:, across[0] * n : (across[-1] + 1) * n])
        for a, i in enumerate(down):
            for b, j in enumerate(across):
                products[i, j] = product[part(a), part(b)]

    multiply(blocks, (0, 1), (1, 2))
    multiply(blocks, (2,), (2,))
    multiply(blocks, (0,), (0,))
    for i, j in ((0, 2), (1, 2), (2, 2), (0, 1), (1, 1), (0, 0)):
        value = 3.0 * square[i, j] - 2.0 * products[i, j]
        frame[part(i), part(j)] = value.astype(BF16)
        if i < j:
            frame[part(j), part(i)] = value.astype(BF16).T
    product = dot(frame[: 2 * n, :], frame[:, n:])
    square = {(i, j): product[part(i), part(j - 1)] for i in (0, 1) for j in (1, 2)}
    square[2, 2] = dot(frame[2 * n :, :], frame[:, 2 * n :])
    for (i, j), value in square.items():
        low[part(i), part(j)] = value.astype(BF16)
    low[part(2), part(1)] = square[1, 2].astype(BF16).T
    crossed[0] = square[0, 1].astype(BF16).T
    crossed[1] = square[0, 2].astype(BF16).T
    pieces = []
    for s in (1, 2):
        density = 3.0 * square[s, s] - 2.0 * dot(frame[part(s), :], low[:, part(s)])
        pieces.append(pack(density - members[s - 1]).astype(BF16))
    for at, ref in enumerate(sent):
        value = pieces[0] * rows[at : at + 1, :].astype(BF16)
        if at >= workers - 1:
            value = value + pieces[1] * rows[at + workers : at + workers + 1, :].astype(BF16)
        ref[0] = value


def own_kernel(own, frame, crossed, mine, delta):
    n = mine.shape[-1]
    delta[...] = own[...].astype(F32) - purified(own[...])
    square = dot(frame[:n, :], frame[:, :n])
    low = jnp.concatenate([square.astype(BF16), crossed[0], crossed[1]], 0)
    mine[...] = 3.0 * square - 2.0 * dot(frame[:n, :], low)


def add_kernel(*refs):
    *parts, out = refs
    total = parts[0][...].astype(F32)
    for ref in parts[1:]:
        total = total + ref[...].astype(F32)
    out[...] = total.astype(BF16)


def finish_kernel(*refs):
    *packed, mine, delta, out = refs
    n = mine.shape[-1]
    half = n // 2
    total = packed[0][0].astype(F32)
    for ref in packed[1:]:
        total = total + ref[0].astype(F32)
    count = total[n + 1 : n + 2, :]
    top, bottom = slice(0, half), slice(half, n)
    for value, down, across in zip(unpack(total), (top, top, bottom, bottom), (top, bottom, top, bottom)):
        out[0, down, across] = mine[down, across] + count * delta[down, across] + value


def in_hbm(array):
    return pltpu.with_memory_space_constraint(array, pltpu.HBM)


def call(kernel, operands, outs, flops=0, scratch=(), distant=0, limit=24):
    vmem = pl.BlockSpec(memory_space=pltpu.VMEM)
    return pl.pallas_call(
        kernel,
        in_specs=[pl.BlockSpec(memory_space=pltpu.HBM)] * distant + [vmem] * (len(operands) - distant),
        out_specs=[vmem] * len(outs),
        out_shape=[jax.ShapeDtypeStruct(*out) for out in outs],
        scratch_shapes=scratch,
        cost_estimate=pl.CostEstimate(flops=flops, bytes_accessed=0, transcendentals=0),
        compiler_params=pltpu.CompilerParams(vmem_limit_bytes=limit * 1024 * 1024),
    )(*operands)


def step(mono_ham, polymer_members, polymer_coupling):
    workers = lax.axis_size("wrk")
    groups = lax.axis_size("grp")
    n = mono_ham.shape[-1]
    tall, wide = n + PAD, n // 2
    packed, own = call(pack_kernel, (mono_ham,), [((1, tall, wide), BF16), ((n, n), BF16)], flops=1000)
    candidates = gather(packed)
    frame, known, rows = call(
        functools.partial(early_kernel, workers=workers, groups=groups),
        (in_hbm(polymer_members), in_hbm(polymer_coupling), own),
        [((3 * n, 3 * n), BF16), ((3 * n, 3 * n), F32), ((3 * workers - 1, wide), F32)],
        flops=2 * 18 * n**3,
        distant=2,
        scratch=[
            pltpu.VMEM(polymer_members.shape, jnp.int32),
            pltpu.VMEM(polymer_coupling.shape, BF16),
            pltpu.SemaphoreType.DMA((2,)),
        ],
    )
    targets = everyone(workers)
    *sent, frame, crossed = call(
        functools.partial(main_kernel, workers=workers),
        candidates + [frame, known, rows],
        [((1, tall, wide), BF16)] * len(targets) + [((3 * n, 3 * n), BF16), ((2, n, n), BF16)],
        flops=2 * 45 * n**3,
        scratch=[pltpu.VMEM((3 * n, 3 * n), BF16)],
    )
    received = give_back(dict(zip(targets, sent)))
    mine, delta = call(own_kernel, (own, frame, crossed), [((n, n), F32)] * 2, flops=2 * 10 * n**3)
    (density,) = call(finish_kernel, received + [mine, delta], [((1, n, n), F32)], flops=1000)
    return density


def solution(mesh):
    placed = (
        P(("grp", "wrk"), None, None),
        P(("grp", "wrk"), None),
        P(("grp", "wrk"), None, None, None),
    )
    return jax.shard_map(step, mesh=mesh, in_specs=placed, out_specs=P(("grp", "wrk"), None, None), check_vma=False)
```

```python
import functools

import jax
import jax.numpy as jnp
from jax import lax
from jax.experimental import pallas as pl
from jax.experimental.pallas import tpu as pltpu
from jax.sharding import PartitionSpec as P


F32 = jnp.float32
BF16 = jnp.bfloat16
PAD = 8


def mate(slot, k, workers):
    return slot ^ k if workers == 4 else lax.rem(slot + k, workers)


def pairs(distance, k):
    groups, workers = lax.axis_size("grp"), lax.axis_size("wrk")
    for g in range(groups):
        for w in range(workers):
            other = w ^ k if workers == 4 else (w + k) % workers
            yield g * workers + w, (g + distance) % groups * workers + other


def from_mate(block, distance, k):
    return lax.ppermute(block, ("grp", "wrk"), [(there, here) for here, there in pairs(distance, k)])


def to_mate(block, distance, k):
    return lax.ppermute(block, ("grp", "wrk"), list(pairs(distance, k)))


def everyone(workers):
    return [(0, k) for k in range(1, workers)] + [(1, k) for k in range(workers)]


def gather_plan(workers):
    if workers == 4:
        return [(0, 2, None), (0, 1, None), (1, 1, None), (1, 0, None), (0, 1, 2), (1, 0, 2), (1, 1, 2)]
    return [(distance, k, None) for distance, k in everyone(workers)]


def gather(packed):
    blocks = {}
    for distance, k, what in gather_plan(lax.axis_size("wrk")):
        sent = packed if what is None else blocks[0, what]
        blocks[distance, k ^ (what or 0)] = from_mate(sent, distance, k)
    return [blocks[at] for at in everyone(lax.axis_size("wrk"))]


def return_plan(workers):
    if workers == 4:
        return [(1, 1, 3), (1, 0, 2), (0, 1, 3), (1, 0, 0), (1, 1, 1), (0, 1, 1)]
    return [(distance, k, k) for distance, k in everyone(workers)]


def give_back(pieces):
    workers = lax.axis_size("wrk")
    near, far = [], []
    for distance, k, owner in return_plan(workers):
        block = to_mate(pieces[distance, owner], distance, k)
        (near if k == owner else far).append(block)
    if far:
        (total,) = call(add_kernel, far + [pieces[0, 2]], [(far[0].shape, BF16)], flops=1000)
        near.append(to_mate(total, 0, 2))
    return near


def dot(a, b):
    return jnp.dot(a, b, preferred_element_type=F32)


def grid_masks(half):
    row = lax.broadcasted_iota(jnp.int32, (half, half), 0)
    col = lax.broadcasted_iota(jnp.int32, (half, half), 1)
    return row, col


def eye(n):
    row, col = grid_masks(n)
    return jnp.where(row == col, 1.0, 0.0)


def pack(block):
    n = block.shape[-1]
    half = n // 2
    row, col = grid_masks(half)
    low = block[half:, half:]
    folded = jnp.where(row >= col, block[:half, :half], low)
    diagonal = jnp.sum(jnp.where(row == col, low, 0.0), axis=0, keepdims=True)
    line = lax.broadcasted_iota(jnp.int32, (PAD, half), 0)
    tail = jnp.where(line == 0, diagonal, 1.0)
    return jnp.concatenate([folded, block[:half, half:], tail], 0)


def unpack(packed):
    half = packed.shape[-1]
    folded, corner, diagonal = packed[:half], packed[half : 2 * half], packed[2 * half : 2 * half + 1]
    row, col = grid_masks(half)
    turned = folded.T
    first = jnp.where(row >= col, folded, turned)
    last = jnp.where(row < col, folded, jnp.where(row > col, turned, diagonal))
    return first, corner, corner.T, last


def purified(low):
    square = dot(low, low)
    density = 3.0 * square - 2.0 * dot(square.astype(BF16), low)
    low = density.astype(BF16)
    square = dot(low, low)
    return 3.0 * square - 2.0 * dot(square.astype(BF16), low)


def pack_kernel(ham, out, own):
    n = ham.shape[-1]
    block = 0.5 * eye(n) - 0.35 * ham[0].astype(F32)
    out[0] = pack(block).astype(BF16)
    own[...] = block.astype(BF16)


def early_kernel(
    members_hbm, coupling_hbm, own_ref, frame, known, rows, members, coupling, arrived, *, workers, groups
):
    n = own_ref.shape[-1]
    listing = pltpu.make_async_copy(members_hbm, members, arrived.at[0])
    fetch = pltpu.make_async_copy(coupling_hbm, coupling, arrived.at[1])
    listing.start()
    fetch.start()
    listing.wait()
    group = lax.axis_index("grp")
    slot = lax.axis_index("wrk")
    following = lax.rem(group + 1, groups)
    second, last = members[:, 1:2], members[:, 2:3]
    line = 0

    def put(value):
        nonlocal line
        rows[line : line + 1, :] = jnp.broadcast_to(value, (1, n // 2)).astype(F32)
        line += 1

    def hit(member, member_group, member_slot):
        return jnp.where(member == member_group * workers + member_slot, 1.0, 0.0)

    for k in range(1, workers):
        put(hit(second, group, mate(slot, k, workers)))
    for member in (second, last):
        for k in range(workers):
            put(hit(member, following, mate(slot, k, workers)))
    own = own_ref[...]
    third = jnp.where(last >= 0, 1.0, 0.0)
    fetch.wait()
    c01 = -0.35 * coupling[0, 0].astype(F32)
    c02 = -0.35 * coupling[0, 1].astype(F32) * third
    c12 = -0.35 * coupling[0, 2].astype(F32) * third
    frame[:n, :n] = own
    frame[:n, n : 2 * n] = c01.astype(BF16)
    frame[:n, 2 * n :] = c02.astype(BF16)
    frame[n : 2 * n, :n] = c01.T.astype(BF16)
    frame[n : 2 * n, n : 2 * n] = jnp.zeros((n, n), BF16)
    frame[n : 2 * n, 2 * n :] = c12.astype(BF16)
    frame[2 * n :, :n] = c02.T.astype(BF16)
    frame[2 * n :, n : 2 * n] = c12.T.astype(BF16)
    frame[2 * n :, 2 * n :] = jnp.zeros((n, n), BF16)
    known[:n, :n] = dot(frame[:n, :], frame[:, :n])
    known[:, 2 * n :] = dot(frame[:, : 2 * n], frame[: 2 * n, 2 * n :])
    left = dot(frame[: 2 * n, :n], frame[:n, n : 2 * n])
    known[: 2 * n, n : 2 * n] = left + dot(frame[: 2 * n, 2 * n :], frame[2 * n :, n : 2 * n])


def main_kernel(*refs, workers):
    own = refs[: workers - 1]
    following = refs[workers - 1 : 2 * workers - 1]
    first, known, rows = refs[2 * workers - 1 : 2 * workers + 2]
    sent = refs[2 * workers + 2 : -3]
    frame, crossed, low = refs[-3:]
    n = known.shape[-1] // 3
    half = n // 2

    def part(i):
        return slice(i * n, (i + 1) * n)

    def chosen(candidates, first_row):
        total = jnp.zeros((n + PAD, half), F32)
        for c, ref in enumerate(candidates):
            total = jnp.where(rows[first_row + c : first_row + c + 1, :] > 0.5, ref[0].astype(F32), total)
        return total

    members = []
    for packed in (chosen(own + following, 0), chosen(following, 2 * workers - 1)):
        a, b, c, d = unpack(packed)
        block = jnp.concatenate([jnp.concatenate([a, b], 1), jnp.concatenate([c, d], 1)], 0)
        members.append(block)
    second, last = [block.astype(BF16) for block in members]
    blocks = {(i, j): first[part(i), part(j)] for i in range(3) for j in range(3)}
    blocks[1, 1], blocks[2, 2] = second, last

    def rectangle(table, down, across):
        return jnp.concatenate([jnp.concatenate([table[i, j] for j in across], 1) for i in down], 0)

    square = {(i, j): known[part(i), part(j)] for j in range(3) for i in range(j + 1)}
    extra = dot(rectangle(blocks, (0, 1), (1,)), second)
    square[0, 1] += extra[:n]
    square[1, 1] += extra[n:]
    extra = dot(rectangle(blocks, (0, 1, 2), (2,)), last)
    square[0, 2] += extra[:n]
    square[1, 2] += extra[n : 2 * n] + dot(second, blocks[1, 2])
    square[2, 2] += extra[2 * n :]
    for (i, j), value in square.items():
        low[part(i), part(j)] = value.astype(BF16)
        if i < j:
            low[part(j), part(i)] = value.T.astype(BF16)
    products = {}

    def multiply(table, down, across):
        product = dot(rectangle(table, down, range(3)), low[:, across[0] * n : (across[-1] + 1) * n])
        for a, i in enumerate(down):
            for b, j in enumerate(across):
                products[i, j] = product[part(a), part(b)]

    multiply(blocks, (0, 1), (1, 2))
    multiply(blocks, (2,), (2,))
    multiply(blocks, (0,), (0,))
    for i, j in ((0, 2), (1, 2), (2, 2), (0, 1), (1, 1), (0, 0)):
        value = 3.0 * square[i, j] - 2.0 * products[i, j]
        frame[part(i), part(j)] = value.astype(BF16)
        if i < j:
            frame[part(j), part(i)] = value.T.astype(BF16)
    product = dot(frame[: 2 * n, :], frame[:, n:])
    square = {(i, j): product[part(i), part(j - 1)] for i in (0, 1) for j in (1, 2)}
    square[2, 2] = dot(frame[2 * n :, :], frame[:, 2 * n :])
    for (i, j), value in square.items():
        low[part(i), part(j)] = value.astype(BF16)
    low[part(2), part(1)] = square[1, 2].T.astype(BF16)
    crossed[0] = square[0, 1].T.astype(BF16)
    crossed[1] = square[0, 2].T.astype(BF16)
    pieces = []
    for s in (1, 2):
        density = 3.0 * square[s, s] - 2.0 * dot(frame[part(s), :], low[:, part(s)])
        pieces.append(pack(density - members[s - 1]))
    for at, ref in enumerate(sent):
        value = jnp.where(rows[at : at + 1, :] > 0.5, pieces[0], 0.0)
        if at >= workers - 1:
            value = jnp.where(rows[at + workers : at + workers + 1, :] > 0.5, pieces[1], value)
        ref[0] = value.astype(BF16)


def own_kernel(own, frame, crossed, mine, delta):
    n = mine.shape[-1]
    delta[...] = own[...].astype(F32) - purified(own[...])
    square = dot(frame[:n, :], frame[:, :n])
    low = jnp.concatenate([square.astype(BF16), crossed[0], crossed[1]], 0)
    mine[...] = 3.0 * square - 2.0 * dot(frame[:n, :], low)


def add_kernel(*refs):
    *parts, out = refs
    total = parts[0][...].astype(F32)
    for ref in parts[1:]:
        total = total + ref[...].astype(F32)
    out[...] = total.astype(BF16)


def finish_kernel(*refs):
    *packed, mine, delta, out = refs
    n = mine.shape[-1]
    half = n // 2
    total = packed[0][0].astype(F32)
    for ref in packed[1:]:
        total = total + ref[0].astype(F32)
    count = total[n + 1 : n + 2, :]
    top, bottom = slice(0, half), slice(half, n)
    for value, down, across in zip(unpack(total), (top, top, bottom, bottom), (top, bottom, top, bottom)):
        out[0, down, across] = mine[down, across] + count * delta[down, across] + value


def in_hbm(array):
    return pltpu.with_memory_space_constraint(array, pltpu.HBM)


def call(kernel, operands, outs, flops=0, scratch=(), distant=0, limit=24):
    vmem = pl.BlockSpec(memory_space=pltpu.VMEM)
    return pl.pallas_call(
        kernel,
        in_specs=[pl.BlockSpec(memory_space=pltpu.HBM)] * distant + [vmem] * (len(operands) - distant),
        out_specs=[vmem] * len(outs),
        out_shape=[jax.ShapeDtypeStruct(*out) for out in outs],
        scratch_shapes=scratch,
        cost_estimate=pl.CostEstimate(flops=flops, bytes_accessed=0, transcendentals=0),
        compiler_params=pltpu.CompilerParams(vmem_limit_bytes=limit * 1024 * 1024),
    )(*operands)


def step(mono_ham, polymer_members, polymer_coupling):
    workers = lax.axis_size("wrk")
    groups = lax.axis_size("grp")
    n = mono_ham.shape[-1]
    tall, wide = n + PAD, n // 2
    packed, own = call(pack_kernel, (mono_ham,), [((1, tall, wide), BF16), ((n, n), BF16)], flops=1000)
    candidates = gather(packed)
    frame, known, rows = call(
        functools.partial(early_kernel, workers=workers, groups=groups),
        (in_hbm(polymer_members), in_hbm(polymer_coupling), own),
        [((3 * n, 3 * n), BF16), ((3 * n, 3 * n), F32), ((3 * workers - 1, wide), F32)],
        flops=2 * 18 * n**3,
        distant=2,
        scratch=[
            pltpu.VMEM(polymer_members.shape, jnp.int32),
            pltpu.VMEM(polymer_coupling.shape, BF16),
            pltpu.SemaphoreType.DMA((2,)),
        ],
    )
    targets = everyone(workers)
    *sent, frame, crossed = call(
        functools.partial(main_kernel, workers=workers),
        candidates + [frame, known, rows],
        [((1, tall, wide), BF16)] * len(targets) + [((3 * n, 3 * n), BF16), ((2, n, n), BF16)],
        flops=2 * 45 * n**3,
        scratch=[pltpu.VMEM((3 * n, 3 * n), BF16)],
    )
    received = give_back(dict(zip(targets, sent)))
    mine, delta = call(own_kernel, (own, frame, crossed), [((n, n), F32)] * 2, flops=2 * 10 * n**3)
    (density,) = call(finish_kernel, received + [mine, delta], [((1, n, n), F32)], flops=1000)
    return density


def solution(mesh):
    placed = (
        P(("grp", "wrk"), None, None),
        P(("grp", "wrk"), None),
        P(("grp", "wrk"), None, None, None),
    )
    return jax.shard_map(step, mesh=mesh, in_specs=placed, out_specs=P(("grp", "wrk"), None, None), check_vma=False)
```
